32 devices in a mesh: ez: 4 (over z), ey: 2 (over y), ex: 4 (over x, core).
Axes of the slice: x: 2, y: 2, z: 4, core: 2. Of those that a mesh axis runs over, the one named last changes fastest.
Arguments:
- x_tokens: bfloat16 [16384, 2048], P(('ez', 'ey', 'ex'))
- expert_ids: int32 [16384, 4], P(('ez', 'ey', 'ex'))
- gate_vals: float32 [16384, 4], P(('ez', 'ey', 'ex'))
- w_gate: bfloat16 [32, 2048, 1792], P(('ex', 'ey', 'ez'))
- w_up: bfloat16 [32, 2048, 1792], P(('ex', 'ey', 'ez'))
- w_down: bfloat16 [32, 1792, 2048], P(('ex', 'ey', 'ez'))
Outputs:
- output: bfloat16 [16384, 2048], P(('ez', 'ey', 'ex'))
All inputs are finite; a program needn't handle non-finite values.
Results may differ from the reference program's by a relative error of at most 0.00585087.
Values are sent between devices in bfloat16 or wider.
A program may use at most 1 GiB of HBM per device.

```python
import jax
import jax.numpy as jnp
from jax import lax

HIDDEN = 2048
FFN_DIM = 1792
EXPERTS = 32
TOP_K = 4
TOK_DEV = 512
DEVICES = 32
GROUPS = 8

TOKENS_ALL = DEVICES * TOK_DEV
CAP_EXPERT = 2 * DEVICES * TOK_DEV * TOP_K // EXPERTS


def draw_routing(route_key):
    perm_key, group_key = jax.random.split(route_key)
    group_size = EXPERTS // GROUPS
    pair_count = group_size // 2
    pick_groups = TOP_K // 2
    perm_score = jax.random.randint(perm_key, (DEVICES, GROUPS, group_size), 0, 1 << 20)
    inner_perm = jnp.argsort(perm_score * group_size + jnp.arange(group_size), axis=-1)
    inner_perm = inner_perm.at[:, :, 2].set(inner_perm[:, :, 0])
    group_score = jax.random.randint(group_key, (DEVICES, GROUPS), 0, 1 << 20)
    group_perm = jnp.argsort(group_score * GROUPS + jnp.arange(GROUPS), axis=-1)
    visit_idx = jnp.arange(TOK_DEV)[:, None] * pick_groups + jnp.arange(pick_groups)[None, :]
    dev_idx = jnp.arange(DEVICES)[:, None, None]
    group_id = group_perm[dev_idx, visit_idx[None] % GROUPS]
    pair_pos = 2 * ((visit_idx // GROUPS) % pair_count)[None]
    first_pick = inner_perm[dev_idx, group_id, pair_pos]
    second_pick = inner_perm[dev_idx, group_id, pair_pos + 1]
    local_pick = jnp.stack([first_pick, second_pick], axis=-1)
    expert_ids = group_id[:, :, :, None] * group_size + local_pick
    return expert_ids.reshape(TOKENS_ALL, TOP_K).astype(jnp.int32)


def setup_inputs(seed: int = 0) -> dict:
    base_key = jax.random.key(seed)
    key_x, key_gate, key_one, key_three, key_two, key_route = jax.random.split(base_key, 6)
    x_tokens = jax.random.normal(key_x, (TOKENS_ALL, HIDDEN), jnp.float32)
    gate_raw = jax.random.uniform(key_gate, (TOKENS_ALL, TOP_K), jnp.float32, 0.5, 1.5)
    gate_vals = 2.5 * gate_raw / jnp.sum(gate_raw, axis=1, keepdims=True)
    w_gate = jax.random.normal(key_one, (EXPERTS, HIDDEN, FFN_DIM), jnp.float32) * HIDDEN ** -0.5
    w_up = jax.random.normal(key_three, (EXPERTS, HIDDEN, FFN_DIM), jnp.float32) * HIDDEN ** -0.5
    w_down = jax.random.normal(key_two, (EXPERTS, FFN_DIM, HIDDEN), jnp.float32) * FFN_DIM ** -0.5
    return {
        'x_tokens': x_tokens.astype(jnp.bfloat16),
        'expert_ids': draw_routing(key_route),
        'gate_vals': gate_vals,
        'w_gate': w_gate.astype(jnp.bfloat16),
        'w_up': w_up.astype(jnp.bfloat16),
        'w_down': w_down.astype(jnp.bfloat16),
    }


def reference(x_tokens, expert_ids, gate_vals, w_gate, w_up, w_down):
    flat_ids = expert_ids.reshape(-1)
    flat_gates = gate_vals.reshape(-1)
    pair_tok = jnp.arange(TOKENS_ALL * TOP_K) // TOP_K
    slot_pos = jnp.arange(CAP_EXPERT)

    def expert_step(acc_sum, scan_in):
        expert, w_one, w_three, w_two = scan_in
        chosen = flat_ids == expert
        n_chosen = jnp.sum(chosen.astype(jnp.int32))
        pair_sel = jnp.nonzero(chosen, size=CAP_EXPERT, fill_value=0)[0]
        tok_sel = pair_tok[pair_sel]
        weight = jnp.where(slot_pos < n_chosen, flat_gates[pair_sel], 0.0)
        tok_rows = x_tokens[tok_sel]
        h_gate = jnp.dot(tok_rows, w_one, preferred_element_type=jnp.float32)
        h_up = jnp.dot(tok_rows, w_three, preferred_element_type=jnp.float32)
        act_bf = (jax.nn.silu(h_gate) * h_up).astype(jnp.bfloat16)
        exp_out = jnp.dot(act_bf, w_two, preferred_element_type=jnp.float32).astype(jnp.bfloat16)
        acc_sum = acc_sum.at[tok_sel].add(weight[:, None] * exp_out.astype(jnp.float32))
        return acc_sum, None

    acc_init = jnp.zeros((TOKENS_ALL, HIDDEN), jnp.float32)
    moe_sum = lax.scan(expert_step, acc_init, (jnp.arange(EXPERTS), w_gate, w_up, w_down))[0]
    return (x_tokens.astype(jnp.float32) + moe_sum).astype(jnp.bfloat16)
```

```python
import jax
import jax.numpy as jnp
from jax import lax
from jax.experimental import pallas as pl
from jax.experimental.pallas import tpu as pltpu
from jax.sharding import PartitionSpec as P

TOKEN_AXES = ('ez', 'ey', 'ex')
EXPERT_AXES = ('ex', 'ey', 'ez')
MESH = pl.DeviceIdType.MESH
BF16 = jnp.bfloat16
F32 = jnp.float32
SEND_ORDER = (6, 7, 2, 3, 4, 5, 1)


def tile_of(n):
    return 256 if n % 256 == 0 else 128


def z_peer(k):
    z = lax.axis_index('ez')
    return 2 * ((z // 2 + k // 2) % 2) + (z % 2 + k % 2) % 2


def plane_peer(j):
    y, col = lax.axis_index('ey'), lax.axis_index('ex')
    return (y + j // 4) % 2, 2 * ((col // 2 + (j // 2) % 2) % 2) + (col % 2 + j % 2) % 2


def moe_kernel(x_ref, rkr_ref, rg_ref, w1_ref, w3_ref, w2_ref,
               y_ref, xz_ref, dr_ref, rr_ref, zr_ref,
               w1v, w3v, w2v, gbuf, rbuf, act, xbuf, sel, cmat, pb,
               w_sem, xl_sem, rl_sem, pl_sem, xs_sem, xr_sem, ds_sem, dr_sem, rs_sem, rc_sem, zs_sem, zr_sem):
    tok, hid = x_ref.shape
    ffn = w1_ref.shape[1]
    rows = gbuf.shape[1]
    cap = rows // 8
    half = rows // 2
    pieces = xs_sem.shape[1]
    prow = tok // pieces
    tn, tf = tile_of(hid), tile_of(ffn)
    tt = cmat.shape[1]

    def xcopy(k, p):
        span = pl.ds(p * prow, prow)
        src = xz_ref.at[1, span] if k == 3 else x_ref.at[span]
        return pltpu.make_async_remote_copy(
            src_ref=src, dst_ref=xz_ref.at[k - 1, span], send_sem=xs_sem.at[k, p], recv_sem=xr_sem.at[k, p],
            device_id={'ez': z_peer(1 if k == 3 else k)}, device_id_type=MESH)

    def plane_copy(src, dst, k, j, send, recv):
        span = pl.ds(j * cap, cap)
        if j == 0:
            return pltpu.make_async_copy(src.at[k, span], dst.at[k, span], recv.at[k, 0])
        yy, cc = plane_peer(j)
        return pltpu.make_async_remote_copy(
            src_ref=src.at[k, span], dst_ref=dst.at[k, span], send_sem=send.at[k, j], recv_sem=recv.at[k, j],
            device_id={'ey': yy, 'ex': cc}, device_id_type=MESH)

    def dcopy(k, j):
        return plane_copy(gbuf, dr_ref, k, j, ds_sem, dr_sem)

    def rcopy(k, j):
        return plane_copy(gbuf, rr_ref, k, j, rs_sem, rc_sem)

    def zcopy(slot, i, k):
        return pltpu.make_async_remote_copy(
            src_ref=pb.at[slot], dst_ref=zr_ref.at[i], send_sem=zs_sem.at[i], recv_sem=zr_sem.at[i],
            device_id={'ez': z_peer(k)}, device_id_type=MESH)

    def wait_recv(copy, j):
        if j == 0:
            copy.wait()
        else:
            copy.wait_recv()

    weights = [pltpu.make_async_copy(s, d, w_sem.at[i])
               for i, (s, d) in enumerate(((w1_ref, w1v), (w3_ref, w3v), (w2_ref, w2v)))]

    def load_x(k):
        return pltpu.make_async_copy(x_ref if k == 0 else xz_ref.at[k - 1], xbuf, xl_sem)

    def gather(k):
        load = load_x(k)
        load.start()
        s = z_peer(k)
        for j in range(8):
            slot = lax.broadcasted_iota(jnp.int32, (cap, tok), 0).astype(F32)
            hit = rkr_ref[s, j:j + 1, :] == slot
            sel[j * cap:(j + 1) * cap, :] = jnp.where(hit, 1.0, 0.0).astype(BF16)
        load.wait()

        def body(n, carry):
            cols = pl.ds(pl.multiple_of(n * tn, tn), tn)
            gbuf[k, :, cols] = jnp.dot(sel[...], xbuf[:, cols], preferred_element_type=F32).astype(BF16)
            return carry

        lax.fori_loop(0, hid // tn, body, 0)
        for j in SEND_ORDER + (0,):
            dcopy(k, j).start()

    def expert(k):
        loads = []
        for h in range(2):
            for j in range(4 * h, 4 * h + 4):
                wait_recv(dcopy(k, j), j)
            span = pl.ds(h * half, half)
            loads.append(pltpu.make_async_copy(dr_ref.at[k, span], rbuf.at[span], rl_sem.at[h]))
            loads[h].start()
        for j in range(1, 8):
            dcopy(k, j).wait_send()
        for h in range(2):
            loads[h].wait()
            span = pl.ds(h * half, half)

            def up(n, carry):
                cols = pl.ds(pl.multiple_of(n * tf, tf), tf)
                row = rbuf[span, :]
                one = jnp.dot(row, w1v[:, cols], preferred_element_type=F32)
                three = jnp.dot(row, w3v[:, cols], preferred_element_type=F32)
                act[:, cols] = (one * jax.nn.sigmoid(one) * three).astype(BF16)
                return carry

            lax.fori_loop(0, ffn // tf, up, 0)

            def down(n, carry):
                cols = pl.ds(pl.multiple_of(n * tn, tn), tn)
                gbuf[k, span, cols] = jnp.dot(act[...], w2v[:, cols], preferred_element_type=F32).astype(BF16)
                return carry

            lax.fori_loop(0, hid // tn, down, 0)

    def send_back(k):
        for j in SEND_ORDER + (0,):
            rcopy(k, j).start()

    def combine(k, slot):
        loads = []
        for h in range(2):
            for j in range(4 * h, 4 * h + 4):
                wait_recv(rcopy(k, j), j)
            span = pl.ds(h * half, half)
            loads.append(pltpu.make_async_copy(rr_ref.at[k, span], rbuf.at[span], rl_sem.at[h]))
            loads[h].start()
        s = z_peer(k)
        for t in range(tok // tt):
            span = pl.ds(t * tt, tt)
            info = rg_ref[s, span, :]
            for j in range(8):
                slots = lax.broadcasted_iota(jnp.int32, (tt, cap), 1).astype(F32)
                hit = info[:, j:j + 1] == slots
                left = info[:, 8 + j:9 + j]
                for i in range(3):
                    part = left.astype(BF16).astype(F32)
                    left = left - part
                    cmat[i, :, j * cap:(j + 1) * cap] = jnp.where(hit, part, 0.0).astype(BF16)
            if t == 0:
                for load in loads:
                    load.wait()

            def body(n, carry):
                cols = pl.ds(pl.multiple_of(n * tn, tn), tn)
                back = rbuf[:, cols]
                total = jnp.dot(cmat[2], back, preferred_element_type=F32)
                total = total + jnp.dot(cmat[1], back, preferred_element_type=F32)
                pb[slot, span, cols] = total + jnp.dot(cmat[0], back, preferred_element_type=F32)
                return carry

            lax.fori_loop(0, hid // tn, body, 0)

    for k in (1, 2):
        for p in range(pieces):
            xcopy(k, p).start()
    for w in weights:
        w.start()
    gather(0)
    for p in range(pieces):
        xcopy(1, p).wait_recv()
    gather(1)
    for w in weights:
        w.wait()
    expert(0)
    for p in range(pieces):
        xcopy(2, p).wait_recv()
        xcopy(3, p).start()
    gather(2)
    expert(1)
    for p in range(pieces):
        xcopy(3, p).wait_recv()
    gather(3)
    expert(2)
    expert(3)
    for k in (3, 1, 2, 0):
        send_back(k)
    combine(3, 0)
    zcopy(0, 1, 1).start()
    combine(1, 2)
    zcopy(2, 0, 1).start()
    combine(2, 1)
    zcopy(0, 1, 1).wait()
    near = pltpu.make_async_copy(zr_ref.at[1], pb.at[0], pl_sem.at[0])
    near.start()
    near.wait()

    def row_loop(body):
        step = 16
        lax.fori_loop(0, tok // step, lambda i, c: (body(pl.ds(pl.multiple_of(i * step, step), step)), c)[1], 0)

    def add_near(span):
        pb[1, span, :] += pb[0, span, :]

    row_loop(add_near)
    zcopy(1, 2, 2).start()
    combine(0, 0)
    load = load_x(0)
    load.start()
    load.wait()
    zcopy(2, 0, 1).wait()
    first = pltpu.make_async_copy(zr_ref.at[0], pb.at[2], pl_sem.at[1])
    first.start()
    first.wait()

    def add_first(span):
        pb[0, span, :] += xbuf[span, :].astype(F32) + pb[2, span, :]

    row_loop(add_first)
    zcopy(1, 2, 2).wait()
    last = pltpu.make_async_copy(zr_ref.at[2], pb.at[1], pl_sem.at[0])
    last.start()
    last.wait()

    def add_last(span):
        xbuf[span, :] = (pb[0, span, :] + pb[1, span, :]).astype(BF16)

    row_loop(add_last)
    out = pltpu.make_async_copy(xbuf, y_ref, xl_sem)
    out.start()
    for k in (1, 2, 3):
        for p in range(pieces):
            xcopy(k, p).wait_send()
    for k in range(4):
        for j in range(1, 8):
            rcopy(k, j).wait_send()
    out.wait()


def route(ids, gates):
    tok = ids.shape[0]
    peers = [plane_peer(j) for j in range(8)]
    experts = jnp.stack([(c * 2 + y) * 4 + z for z in range(4) for y, c in peers]).astype(jnp.int32)
    match = ids[:, :, None] == experts[None, None, :]
    picked = jnp.any(match, axis=1)
    gate = jnp.sum(jnp.where(match, gates[:, :, None], 0.0), axis=1)
    at = jnp.arange(tok)
    before = (at[None, :] < at[:, None]).astype(BF16)
    rank = jnp.dot(before, picked.astype(BF16), preferred_element_type=F32)
    rank = jnp.where(picked, rank, -1.0)
    info = jnp.concatenate([rank.reshape(tok, 4, 8), gate.reshape(tok, 4, 8)], axis=2)
    return lax.all_to_all(info.transpose(1, 0, 2), 'ez', 0, 0)


def solution(mesh):
    n_dev = mesh.shape['ez'] * mesh.shape['ey'] * mesh.shape['ex']

    def local_layer(x_loc, ids_loc, gates_loc, w_g, w_u, w_d):
        tok, hid = x_loc.shape
        ffn = w_g.shape[2]
        cap = 2 * tok * ids_loc.shape[1] // n_dev
        rows = 8 * cap
        info = route(ids_loc, gates_loc)
        ranks = info[:, :, :8].transpose(0, 2, 1)
        pieces = 2
        any_spec = pl.BlockSpec(memory_space=pl.ANY)
        vmem_spec = pl.BlockSpec(memory_space=pltpu.VMEM)
        dma = pltpu.SemaphoreType.DMA
        outs = pl.pallas_call(
            moe_kernel,
            out_shape=(
                jax.ShapeDtypeStruct((tok, hid), BF16),
                jax.ShapeDtypeStruct((3, tok, hid), BF16),
                jax.ShapeDtypeStruct((4, rows, hid), BF16),
                jax.ShapeDtypeStruct((4, rows, hid), BF16),
                jax.ShapeDtypeStruct((3, tok, hid), F32),
            ),
            in_specs=[any_spec, vmem_spec, vmem_spec, any_spec, any_spec, any_spec],
            out_specs=(any_spec,) * 5,
            scratch_shapes=[
                pltpu.VMEM((hid, ffn), BF16),
                pltpu.VMEM((hid, ffn), BF16),
                pltpu.VMEM((ffn, hid), BF16),
                pltpu.VMEM((4, rows, hid), BF16),
                pltpu.VMEM((rows, hid), BF16),
                pltpu.VMEM((rows // 2, ffn), BF16),
                pltpu.VMEM((tok, hid), BF16),
                pltpu.VMEM((rows, tok), BF16),
                pltpu.VMEM((3, tok // 2, rows), BF16),
                pltpu.VMEM((3, tok, hid), F32),
                dma((3,)), dma, dma((2,)), dma((2,)),
                dma((4, pieces)), dma((4, pieces)),
                dma((4, 8)), dma((4, 8)), dma((4, 8)), dma((4, 8)),
                dma((3,)), dma((3,)),
            ],
            compiler_params=pltpu.CompilerParams(has_side_effects=True, vmem_limit_bytes=67043328),
        )(x_loc, ranks, info, w_g[0], w_u[0], w_d[0])
        return outs[0]

    tok_spec = P(TOKEN_AXES, None)
    w_spec = P(EXPERT_AXES, None, None)
    return jax.shard_map(local_layer, mesh=mesh, in_specs=(tok_spec, tok_spec, tok_spec, w_spec, w_spec, w_spec), out_specs=tok_spec, check_vma=False)
```

```python
import jax
import jax.numpy as jnp
from jax import lax
from jax.experimental import pallas as pl
from jax.experimental.pallas import tpu as pltpu
from jax.sharding import PartitionSpec as P

TOKEN_AXES = ('ez', 'ey', 'ex')
EXPERT_AXES = ('ex', 'ey', 'ez')
MESH = pl.DeviceIdType.MESH
BF16 = jnp.bfloat16
F32 = jnp.float32
OFFSET = (0, 1, 2, 4, 3, 5, 6, 7)
HALVES = ((2, 3, 1, 0), (4, 5, 6, 7))


def tile_of(n):
    return 256 if n % 256 == 0 else 128


def z_peer(k):
    z = lax.axis_index('ez')
    return 2 * ((z // 2 + k // 2) % 2) + (z % 2 + k % 2) % 2


def plane_peer(j):
    y, col = lax.axis_index('ey'), lax.axis_index('ex')
    j = OFFSET[j]
    return (y + j // 4) % 2, 2 * ((col // 2 + (j // 2) % 2) % 2) + (col % 2 + j % 2) % 2


def moe_kernel(x_ref, rkr_ref, rg_ref, w1_ref, w3_ref, w2_ref,
               y_ref, xz_ref, dr_ref, rr_ref, zr_ref,
               w1v, w3v, w2v, gbuf, rbuf, act, xbuf, sel, cmat, pb,
               w_sem, xl_sem, rl_sem, pl_sem, xs_sem, xr_sem, ds_sem, dr_sem, rs_sem, rc_sem, zs_sem, zr_sem, out_sem):
    tok, hid = x_ref.shape
    ffn = w1_ref.shape[1]
    rows = gbuf.shape[1]
    cap = rows // 8
    half = rows // 2
    pieces = xs_sem.shape[1]
    prow = tok // pieces
    tn, tf = tile_of(hid), tile_of(ffn)
    tt = cmat.shape[1]
    parts = tok // tt
    z = lax.axis_index('ez')
    inner = ((z + 1) // 2) % 2
    first, second = 1 + inner, 2 - inner

    def xcopy(k, p):
        span = pl.ds(p * prow, prow)
        src = xz_ref.at[1, span] if k == 3 else x_ref.at[span]
        return pltpu.make_async_remote_copy(
            src_ref=src, dst_ref=xz_ref.at[k - 1, span], send_sem=xs_sem.at[k, p], recv_sem=xr_sem.at[k, p],
            device_id={'ez': z_peer(1 if k == 3 else k)}, device_id_type=MESH)

    def plane_copy(src, dst, k, j, send, recv):
        span = pl.ds(j * cap, cap)
        if j == 0:
            return pltpu.make_async_copy(src.at[k, span], dst.at[k, span], recv.at[k, 0])
        yy, cc = plane_peer(j)
        return pltpu.make_async_remote_copy(
            src_ref=src.at[k, span], dst_ref=dst.at[k, span], send_sem=send.at[k, j], recv_sem=recv.at[k, j],
            device_id={'ey': yy, 'ex': cc}, device_id_type=MESH)

    def dcopy(k, j):
        return plane_copy(gbuf, dr_ref, k, j, ds_sem, dr_sem)

    def rcopy(k, j):
        return plane_copy(gbuf, rr_ref, k, j, rs_sem, rc_sem)

    def zcopy(slot, i, k, t):
        span = pl.ds(t * tt, tt)
        return pltpu.make_async_remote_copy(
            src_ref=pb.at[slot, span], dst_ref=zr_ref.at[i, span], send_sem=zs_sem.at[i, t], recv_sem=zr_sem.at[i, t],
            device_id={'ez': z_peer(k)}, device_id_type=MESH)

    def wait_x(k, p):
        span = pl.ds(p * prow, prow)
        pltpu.make_async_remote_copy(
            src_ref=x_ref.at[span], dst_ref=xz_ref.at[k - 1, span], send_sem=xs_sem.at[k, p], recv_sem=xr_sem.at[k, p],
            device_id={'ez': z_peer(k)}, device_id_type=MESH).wait_recv()

    def wait_recv(copy, j):
        if j == 0:
            copy.wait()
        else:
            copy.wait_recv()

    weights = [pltpu.make_async_copy(s, d, w_sem.at[i])
               for i, (s, d) in enumerate(((w1_ref, w1v), (w3_ref, w3v), (w2_ref, w2v)))]

    def load_x(own, k):
        return pltpu.make_async_copy(x_ref if own else xz_ref.at[k - 1], xbuf, xl_sem)

    def gather(k, own=False):
        load = load_x(own, k)
        load.start()
        s = z_peer(k)
        for j in range(8):
            slot = lax.broadcasted_iota(jnp.int32, (cap, tok), 0).astype(F32)
            hit = rkr_ref[s, j:j + 1, :] == slot
            sel[j * cap:(j + 1) * cap, :] = jnp.where(hit, 1.0, 0.0).astype(BF16)
        load.wait()

        def body(n, carry):
            cols = pl.ds(pl.multiple_of(n * tn, tn), tn)
            gbuf[k, :, cols] = jnp.dot(sel[...], xbuf[:, cols], preferred_element_type=F32).astype(BF16)
            return carry

        lax.fori_loop(0, hid // tn, body, 0)
        for j in HALVES[0] + HALVES[1]:
            dcopy(k, j).start()

    def expert(k, send=False):
        loads = []
        for h in range(2):
            for j in range(4 * h, 4 * h + 4):
                wait_recv(dcopy(k, j), j)
            span = pl.ds(h * half, half)
            loads.append(pltpu.make_async_copy(dr_ref.at[k, span], rbuf.at[span], rl_sem.at[h]))
            loads[h].start()
        for j in range(1, 8):
            dcopy(k, j).wait_send()
        for h in range(2):
            loads[h].wait()
            span = pl.ds(h * half, half)

            def up(n, carry):
                cols = pl.ds(pl.multiple_of(n * tf, tf), tf)
                row = rbuf[span, :]
                one = jnp.dot(row, w1v[:, cols], preferred_element_type=F32)
                three = jnp.dot(row, w3v[:, cols], preferred_element_type=F32)
                act[:, cols] = (one * jax.nn.sigmoid(one) * three).astype(BF16)
                return carry

            lax.fori_loop(0, ffn // tf, up, 0)

            def down(n, carry):
                cols = pl.ds(pl.multiple_of(n * tn, tn), tn)
                gbuf[k, span, cols] = jnp.dot(act[...], w2v[:, cols], preferred_element_type=F32).astype(BF16)
                return carry

            lax.fori_loop(0, hid // tn, down, 0)
            if send:
                send_back(k, h)

    def send_back(k, h):
        for j in HALVES[h]:
            rcopy(k, j).start()

    def combine(k, slot, then, done):
        s = z_peer(k)
        loads = []
        for t in range(parts):
            span = pl.ds(t * tt, tt)
            info = rg_ref[s, span, :]
            for j in range(8):
                slots = lax.broadcasted_iota(jnp.int32, (tt, cap), 1).astype(F32)
                hit = info[:, j:j + 1] == slots
                left = info[:, 8 + j:9 + j]
                for i in range(3):
                    part = left.astype(BF16).astype(F32)
                    left = left - part
                    cmat[i, :, j * cap:(j + 1) * cap] = jnp.where(hit, part, 0.0).astype(BF16)
            if t == 0:
                for h in range(2):
                    for j in range(4 * h, 4 * h + 4):
                        wait_recv(rcopy(k, j), j)
                    rspan = pl.ds(h * half, half)
                    loads.append(pltpu.make_async_copy(rr_ref.at[k, rspan], rbuf.at[rspan], rl_sem.at[h]))
                    loads[h].start()
                then()
                for load in loads:
                    load.wait()

            def body(n, carry):
                cols = pl.ds(pl.multiple_of(n * tn, tn), tn)
                back = rbuf[:, cols]
                total = jnp.dot(cmat[2], back, preferred_element_type=F32)
                total = total + jnp.dot(cmat[1], back, preferred_element_type=F32)
                pb[slot, span, cols] = total + jnp.dot(cmat[0], back, preferred_element_type=F32)
                return carry

            lax.fori_loop(0, hid // tn, body, 0)
            done(t)

    def row_loop(t, body):
        step = 16
        lax.fori_loop(
            0, tt // step, lambda i, c: (body(pl.ds(pl.multiple_of(t * tt + i * step, step), step)), c)[1], 0)

    def fetch(i, slot, t):
        span = pl.ds(t * tt, tt)
        return pltpu.make_async_copy(zr_ref.at[i, span], pb.at[slot, span], pl_sem.at[t])

    @pl.when(inner == 0)
    def _():
        for p in range(pieces):
            xcopy(2, p).start()

    for p in range(pieces):
        xcopy(1, p).start()
    for w in weights:
        w.start()
    gather(0, own=True)
    for p in range(pieces):
        wait_x(first, p)

    @pl.when(inner == 1)
    def _():
        for p in range(pieces):
            xcopy(2, p).start()

    gather(first)
    for w in weights:
        w.wait()
    expert(0)
    for p in range(pieces):
        wait_x(second, p)
        xcopy(3, p).start()
    gather(second)
    expert(first)
    for p in range(pieces):
        wait_x(3, p)
    gather(3)
    expert(second)
    expert(3, send=True)

    def back(k):
        return lambda: [send_back(k, h) for h in range(2)] and None

    combine(3, 0, back(1), lambda t: zcopy(0, 1, 1, t).start())
    combine(1, 2, back(2), lambda t: zcopy(2, 0, 1, t).start())

    def pass_on(t):
        zcopy(0, 1, 1, t).wait()
        near = fetch(1, 0, t)
        near.start()
        near.wait()

        def add_near(span):
            pb[1, span, :] += pb[0, span, :]

        row_loop(t, add_near)
        zcopy(1, 2, 2, t).start()

    combine(2, 1, back(0), pass_on)
    load = load_x(True, 0)
    load.start()
    combine(0, 0, lambda: None, lambda t: None)
    load.wait()
    for t in range(parts):
        zcopy(2, 0, 1, t).wait()
        near = fetch(0, 2, t)
        near.start()
        near.wait()

        def add_first(span):
            pb[0, span, :] += xbuf[span, :].astype(F32) + pb[2, span, :]

        row_loop(t, add_first)

    def out(t):
        span = pl.ds(t * tt, tt)
        return pltpu.make_async_copy(xbuf.at[span], y_ref.at[span], out_sem.at[t])

    for t in range(parts):
        zcopy(1, 2, 2, t).wait()
        last = fetch(2, 1, t)
        last.start()
        last.wait()

        def add_last(span):
            xbuf[span, :] = (pb[0, span, :] + pb[1, span, :]).astype(BF16)

        row_loop(t, add_last)
        out(t).start()
    for k in (1, 2, 3):
        for p in range(pieces):
            xcopy(k, p).wait_send()
    for k in range(4):
        for j in range(1, 8):
            rcopy(k, j).wait_send()
    for t in range(parts):
        out(t).wait()


def route(ids, gates):
    tok = ids.shape[0]
    peers = [plane_peer(j) for j in range(8)]
    experts = jnp.stack([(c * 2 + y) * 4 + z for z in range(4) for y, c in peers]).astype(jnp.int32)
    match = ids[:, :, None] == experts[None, None, :]
    picked = jnp.any(match, axis=1)
    gate = jnp.sum(jnp.where(match, gates[:, :, None], 0.0), axis=1)
    at = jnp.arange(tok)
    before = (at[None, :] < at[:, None]).astype(BF16)
    rank = jnp.dot(before, picked.astype(BF16), preferred_element_type=F32)
    rank = jnp.where(picked, rank, -1.0)
    info = jnp.concatenate([rank.reshape(tok, 4, 8), gate.reshape(tok, 4, 8)], axis=2)
    return lax.all_to_all(info.transpose(1, 0, 2), 'ez', 0, 0)


def solution(mesh):
    n_dev = mesh.shape['ez'] * mesh.shape['ey'] * mesh.shape['ex']

    def local_layer(x_loc, ids_loc, gates_loc, w_g, w_u, w_d):
        tok, hid = x_loc.shape
        ffn = w_g.shape[2]
        cap = 2 * tok * ids_loc.shape[1] // n_dev
        rows = 8 * cap
        info = route(ids_loc, gates_loc)
        ranks = info[:, :, :8].transpose(0, 2, 1)
        pieces = 2
        any_spec = pl.BlockSpec(memory_space=pl.ANY)
        vmem_spec = pl.BlockSpec(memory_space=pltpu.VMEM)
        dma = pltpu.SemaphoreType.DMA
        outs = pl.pallas_call(
            moe_kernel,
            out_shape=(
                jax.ShapeDtypeStruct((tok, hid), BF16),
                jax.ShapeDtypeStruct((3, tok, hid), BF16),
                jax.ShapeDtypeStruct((4, rows, hid), BF16),
                jax.ShapeDtypeStruct((4, rows, hid), BF16),
                jax.ShapeDtypeStruct((3, tok, hid), F32),
            ),
            in_specs=[any_spec, vmem_spec, vmem_spec, any_spec, any_spec, any_spec],
            out_specs=(any_spec,) * 5,
            scratch_shapes=[
                pltpu.VMEM((hid, ffn), BF16),
                pltpu.VMEM((hid, ffn), BF16),
                pltpu.VMEM((ffn, hid), BF16),
                pltpu.VMEM((4, rows, hid), BF16),
                pltpu.VMEM((rows, hid), BF16),
                pltpu.VMEM((rows // 2, ffn), BF16),
                pltpu.VMEM((tok, hid), BF16),
                pltpu.VMEM((rows, tok), BF16),
                pltpu.VMEM((3, tok // 2, rows), BF16),
                pltpu.VMEM((3, tok, hid), F32),
                dma((3,)), dma, dma((2,)), dma((2,)),
                dma((4, pieces)), dma((4, pieces)),
                dma((4, 8)), dma((4, 8)), dma((4, 8)), dma((4, 8)),
                dma((3, 2)), dma((3, 2)), dma((2,)),
            ],
            compiler_params=pltpu.CompilerParams(has_side_effects=True, vmem_limit_bytes=67043328),
        )(x_loc, ranks, info, w_g[0], w_u[0], w_d[0])
        return outs[0]

    tok_spec = P(TOKEN_AXES, None)
    w_spec = P(EXPERT_AXES, None, None)
    return jax.shard_map(local_layer, mesh=mesh, in_specs=(tok_spec, tok_spec, tok_spec, w_spec, w_spec, w_spec), out_specs=tok_spec, check_vma=False)
```

```python
import jax
import jax.numpy as jnp
from jax import lax
from jax.experimental import pallas as pl
from jax.experimental.pallas import tpu as pltpu
from jax.sharding import PartitionSpec as P

TOKEN_AXES = ('ez', 'ey', 'ex')
EXPERT_AXES = ('ex', 'ey', 'ez')
MESH = pl.DeviceIdType.MESH
BF16 = jnp.bfloat16
F32 = jnp.float32
OFFSET = (0, 1, 2, 4, 3, 5, 6, 7)
HALVES = ((2, 3, 1, 0), (4, 5, 6, 7))


def tile_of(n):
    return 256 if n % 256 == 0 else 128


def z_peer(k):
    z = lax.axis_index('ez')
    return 2 * ((z // 2 + k // 2) % 2) + (z % 2 + k % 2) % 2


def plane_peer(j):
    y, col = lax.axis_index('ey'), lax.axis_index('ex')
    j = OFFSET[j]
    return (y + j // 4) % 2, 2 * ((col // 2 + (j // 2) % 2) % 2) + (col % 2 + j % 2) % 2


def moe_kernel(x_ref, rank_ref, info_ref, w1_ref, w3_ref, w2_ref,
               y_ref, xz_ref, dr_ref, rr_ref, zr_ref,
               w1v, w3v, w2v, gbuf, rbuf, act, xbuf, sel, cmat, pb, rank_v, info_v,
               w_sem, xl_sem, rl_sem, pl_sem, xs_sem, xr_sem, ds_sem, dr_sem, rs_sem, rc_sem, zs_sem, zr_sem, out_sem, is_sem, ir_sem):
    tok, hid = x_ref.shape
    ffn = w1_ref.shape[1]
    rows = gbuf.shape[1]
    cap = rows // 8
    half = rows // 2
    pieces = xs_sem.shape[1]
    prow = tok // pieces
    tn, tf = tile_of(hid), tile_of(ffn)
    tt = cmat.shape[1]
    parts = tok // tt
    z = lax.axis_index('ez')
    inner = ((z + 1) // 2) % 2
    first, second = 1 + inner, 2 - inner

    def xcopy(k, p):
        span = pl.ds(p * prow, prow)
        src = xz_ref.at[1, span] if k == 3 else x_ref.at[span]
        return pltpu.make_async_remote_copy(
            src_ref=src, dst_ref=xz_ref.at[k - 1, span], send_sem=xs_sem.at[k, p], recv_sem=xr_sem.at[k, p],
            device_id={'ez': z_peer(1 if k == 3 else k)}, device_id_type=MESH)

    def plane_copy(src, dst, k, j, send, recv):
        span = pl.ds(j * cap, cap)
        if j == 0:
            return pltpu.make_async_copy(src.at[k, span], dst.at[k, span], recv.at[k, 0])
        yy, cc = plane_peer(j)
        return pltpu.make_async_remote_copy(
            src_ref=src.at[k, span], dst_ref=dst.at[k, span], send_sem=send.at[k, j], recv_sem=recv.at[k, j],
            device_id={'ey': yy, 'ex': cc}, device_id_type=MESH)

    def dcopy(k, j):
        return plane_copy(gbuf, dr_ref, k, j, ds_sem, dr_sem)

    def rcopy(k, j):
        return plane_copy(gbuf, rr_ref, k, j, rs_sem, rc_sem)

    def zcopy(slot, i, k, t):
        span = pl.ds(t * tt, tt)
        return pltpu.make_async_remote_copy(
            src_ref=pb.at[slot, span], dst_ref=zr_ref.at[i, span], send_sem=zs_sem.at[i, t], recv_sem=zr_sem.at[i, t],
            device_id={'ez': z_peer(k)}, device_id_type=MESH)

    def route_copy(own, k, i):
        src, dst = ((rank_ref, rank_v), (info_ref, info_v))[i]
        if own:
            return pltpu.make_async_copy(src.at[z], dst.at[0], ir_sem.at[0, i])
        peer = z_peer(k)
        return pltpu.make_async_remote_copy(
            src_ref=src.at[peer], dst_ref=dst.at[k], send_sem=is_sem.at[k, i], recv_sem=ir_sem.at[k, i],
            device_id={'ez': peer}, device_id_type=MESH)

    def wait_route(own, k, i):
        copy = route_copy(own, k, i)
        if own:
            copy.wait()
        else:
            copy.wait_recv()

    def wait_x(k, p):
        span = pl.ds(p * prow, prow)
        pltpu.make_async_remote_copy(
            src_ref=x_ref.at[span], dst_ref=xz_ref.at[k - 1, span], send_sem=xs_sem.at[k, p], recv_sem=xr_sem.at[k, p],
            device_id={'ez': z_peer(k)}, device_id_type=MESH).wait_recv()

    def wait_recv(copy, j):
        if j == 0:
            copy.wait()
        else:
            copy.wait_recv()

    weights = [pltpu.make_async_copy(s, d, w_sem.at[i])
               for i, (s, d) in enumerate(((w1_ref, w1v), (w3_ref, w3v), (w2_ref, w2v)))]

    def load_x(own, k):
        return pltpu.make_async_copy(x_ref if own else xz_ref.at[k - 1], xbuf, xl_sem)

    def gather(k, own=False):
        load = load_x(own, k)
        load.start()
        for i in range(2):
            wait_route(own, k, i)
        for j in range(8):
            slot = lax.broadcasted_iota(jnp.int32, (cap, tok), 0).astype(F32)
            hit = rank_v[k, j:j + 1, :] == slot
            sel[j * cap:(j + 1) * cap, :] = jnp.where(hit, 1.0, 0.0).astype(BF16)
        load.wait()

        def body(n, carry):
            cols = pl.ds(pl.multiple_of(n * tn, tn), tn)
            gbuf[k, :, cols] = jnp.dot(sel[...], xbuf[:, cols], preferred_element_type=F32).astype(BF16)
            return carry

        lax.fori_loop(0, hid // tn, body, 0)
        for j in HALVES[0] + HALVES[1]:
            dcopy(k, j).start()

    def expert(k, send=False):
        loads = []
        for h in range(2):
            for j in range(4 * h, 4 * h + 4):
                wait_recv(dcopy(k, j), j)
            span = pl.ds(h * half, half)
            loads.append(pltpu.make_async_copy(dr_ref.at[k, span], rbuf.at[span], rl_sem.at[h]))
            loads[h].start()
        for j in range(1, 8):
            dcopy(k, j).wait_send()
        for h in range(2):
            loads[h].wait()
            span = pl.ds(h * half, half)

            def up(n, carry):
                cols = pl.ds(pl.multiple_of(n * tf, tf), tf)
                row = rbuf[span, :]
                one = jnp.dot(row, w1v[:, cols], preferred_element_type=F32)
                three = jnp.dot(row, w3v[:, cols], preferred_element_type=F32)
                act[:, cols] = (one * jax.nn.sigmoid(one) * three).astype(BF16)
                return carry

            lax.fori_loop(0, ffn // tf, up, 0)

            def down(n, carry):
                cols = pl.ds(pl.multiple_of(n * tn, tn), tn)
                gbuf[k, span, cols] = jnp.dot(act[...], w2v[:, cols], preferred_element_type=F32).astype(BF16)
                return carry

            lax.fori_loop(0, hid // tn, down, 0)
            if send:
                send_back(k, h)

    def send_back(k, h):
        for j in HALVES[h]:
            rcopy(k, j).start()

    def combine(k, slot, then, done):
        loads = []
        for t in range(parts):
            span = pl.ds(t * tt, tt)
            info = info_v[k, span, :]
            for j in range(8):
                slots = lax.broadcasted_iota(jnp.int32, (tt, cap), 1).astype(F32)
                hit = info[:, j:j + 1] == slots
                left = info[:, 8 + j:9 + j]
                for i in range(3):
                    part = left.astype(BF16).astype(F32)
                    left = left - part
                    cmat[i, :, j * cap:(j + 1) * cap] = jnp.where(hit, part, 0.0).astype(BF16)
            if t == 0:
                for h in range(2):
                    for j in range(4 * h, 4 * h + 4):
                        wait_recv(rcopy(k, j), j)
                    rspan = pl.ds(h * half, half)
                    loads.append(pltpu.make_async_copy(rr_ref.at[k, rspan], rbuf.at[rspan], rl_sem.at[h]))
                    loads[h].start()
                then()
                for load in loads:
                    load.wait()

            def body(n, carry):
                cols = pl.ds(pl.multiple_of(n * tn, tn), tn)
                back = rbuf[:, cols]
                total = jnp.dot(cmat[2], back, preferred_element_type=F32)
                total = total + jnp.dot(cmat[1], back, preferred_element_type=F32)
                pb[slot, span, cols] = total + jnp.dot(cmat[0], back, preferred_element_type=F32)
                return carry

            lax.fori_loop(0, hid // tn, body, 0)
            done(t)

    def row_loop(t, body):
        step = 16
        lax.fori_loop(
            0, tt // step, lambda i, c: (body(pl.ds(pl.multiple_of(t * tt + i * step, step), step)), c)[1], 0)

    def fetch(i, slot, t):
        span = pl.ds(t * tt, tt)
        return pltpu.make_async_copy(zr_ref.at[i, span], pb.at[slot, span], pl_sem.at[t])

    for i in range(2):
        route_copy(True, 0, i).start()
    for k in (1, 2, 3):
        for i in range(2):
            route_copy(False, k, i).start()

    @pl.when(inner == 0)
    def _():
        for p in range(pieces):
            xcopy(2, p).start()

    for p in range(pieces):
        xcopy(1, p).start()
    for w in weights:
        w.start()
    gather(0, own=True)
    for p in range(pieces):
        wait_x(first, p)

    @pl.when(inner == 1)
    def _():
        for p in range(pieces):
            xcopy(2, p).start()

    gather(first)
    for w in weights:
        w.wait()
    expert(0)
    for p in range(pieces):
        wait_x(second, p)
        xcopy(3, p).start()
    gather(second)
    expert(first)
    for p in range(pieces):
        wait_x(3, p)
    gather(3)
    expert(second)
    expert(3, send=True)

    def back(k):
        return lambda: [send_back(k, h) for h in range(2)] and None

    combine(3, 0, back(1), lambda t: zcopy(0, 1, 1, t).start())

    def send_near(t):
        @pl.when(inner == 0)
        def _():
            zcopy(2, 0, 1, t).start()

    combine(1, 2, back(2), send_near)

    def pass_on(t):
        zcopy(0, 1, 1, t).wait()
        near = fetch(1, 0, t)
        near.start()
        near.wait()

        def add_near(span):
            pb[1, span, :] += pb[0, span, :]

        row_loop(t, add_near)
        zcopy(1, 2, 2, t).start()

    combine(2, 1, back(0), pass_on)
    load = load_x(True, 0)
    load.start()
    combine(0, 0, lambda: None, lambda t: None)
    load.wait()

    @pl.when(inner == 1)
    def _():
        for t in range(parts):
            zcopy(1, 2, 2, t).wait_send()
            zcopy(2, 0, 1, t).start()

    for t in range(parts):
        zcopy(2, 0, 1, t).wait()
        near = fetch(0, 2, t)
        near.start()
        near.wait()

        def add_first(span):
            pb[0, span, :] += xbuf[span, :].astype(F32) + pb[2, span, :]

        row_loop(t, add_first)

    def out(t):
        span = pl.ds(t * tt, tt)
        return pltpu.make_async_copy(xbuf.at[span], y_ref.at[span], out_sem.at[t])

    for t in range(parts):
        zcopy(1, 2, 2, t).wait_recv()

        @pl.when(inner == 0)
        def _():
            zcopy(1, 2, 2, t).wait_send()

        last = fetch(2, 1, t)
        last.start()
        last.wait()

        def add_last(span):
            xbuf[span, :] = (pb[0, span, :] + pb[1, span, :]).astype(BF16)

        row_loop(t, add_last)
        out(t).start()
    for k in (1, 2, 3):
        for i in range(2):
            route_copy(False, k, i).wait_send()
        for p in range(pieces):
            xcopy(k, p).wait_send()
    for k in range(4):
        for j in range(1, 8):
            rcopy(k, j).wait_send()
    for t in range(parts):
        out(t).wait()


def route(ids, gates):
    tok = ids.shape[0]
    peers = [plane_peer(j) for j in range(8)]
    experts = jnp.stack([(c * 2 + y) * 4 + z for z in range(4) for y, c in peers]).astype(jnp.int32)
    match = ids[:, :, None] == experts[None, None, :]
    picked = jnp.any(match, axis=1)
    gate = jnp.sum(jnp.where(match, gates[:, :, None], 0.0), axis=1)
    at = jnp.arange(tok)
    before = (at[None, :] < at[:, None]).astype(BF16)
    rank = jnp.dot(before, picked.astype(BF16), preferred_element_type=F32)
    rank = jnp.where(picked, rank, -1.0)
    info = jnp.concatenate([rank.reshape(tok, 4, 8), gate.reshape(tok, 4, 8)], axis=2)
    return info.transpose(1, 0, 2)


def solution(mesh):
    n_dev = mesh.shape['ez'] * mesh.shape['ey'] * mesh.shape['ex']

    def local_layer(x_loc, ids_loc, gates_loc, w_g, w_u, w_d):
        tok, hid = x_loc.shape
        ffn = w_g.shape[2]
        cap = 2 * tok * ids_loc.shape[1] // n_dev
        rows = 8 * cap
        info = route(ids_loc, gates_loc)
        ranks = info[:, :, :8].transpose(0, 2, 1)
        pieces = 2
        any_spec = pl.BlockSpec(memory_space=pl.ANY)
        dma = pltpu.SemaphoreType.DMA
        outs = pl.pallas_call(
            moe_kernel,
            out_shape=(
                jax.ShapeDtypeStruct((tok, hid), BF16),
                jax.ShapeDtypeStruct((3, tok, hid), BF16),
                jax.ShapeDtypeStruct((4, rows, hid), BF16),
                jax.ShapeDtypeStruct((4, rows, hid), BF16),
                jax.ShapeDtypeStruct((3, tok, hid), F32),
            ),
            in_specs=[any_spec] * 6,
            out_specs=(any_spec,) * 5,
            scratch_shapes=[
                pltpu.VMEM((hid, ffn), BF16),
                pltpu.VMEM((hid, ffn), BF16),
                pltpu.VMEM((ffn, hid), BF16),
                pltpu.VMEM((4, rows, hid), BF16),
                pltpu.VMEM((rows, hid), BF16),
                pltpu.VMEM((rows // 2, ffn), BF16),
                pltpu.VMEM((tok, hid), BF16),
                pltpu.VMEM((rows, tok), BF16),
                pltpu.VMEM((3, tok // 2, rows), BF16),
                pltpu.VMEM((3, tok, hid), F32),
                pltpu.VMEM((4, 8, tok), F32),
                pltpu.VMEM((4, tok, 16), F32),
                dma((3,)), dma, dma((2,)), dma((2,)),
                dma((4, pieces)), dma((4, pieces)),
                dma((4, 8)), dma((4, 8)), dma((4, 8)), dma((4, 8)),
                dma((3, 2)), dma((3, 2)), dma((2,)), dma((4, 2)), dma((4, 2)),
            ],
            compiler_params=pltpu.CompilerParams(has_side_effects=True, vmem_limit_bytes=67043328),
        )(x_loc, ranks, info, w_g[0], w_u[0], w_d[0])
        return outs[0]

    tok_spec = P(TOKEN_AXES, None)
    w_spec = P(EXPERT_AXES, None, None)
    return jax.shard_map(local_layer, mesh=mesh, in_specs=(tok_spec, tok_spec, tok_spec, w_spec, w_spec, w_spec), out_specs=tok_spec, check_vma=False)
```
